32 devices in a mesh: blk: 16 (over z, y, core), head: 2 (over x).
Axes of the slice: x: 2, y: 2, z: 4, core: 2. Of those that a mesh axis runs over, the one named last changes fastest.
Arguments:
- queries: bfloat16 [8192, 16, 128], P('blk', 'head'), may hold values from -6 to 6
- out_grad: bfloat16 [8192, 16, 128], P('blk', 'head'), may hold values from -6 to 6
- outputs: bfloat16 [8192, 16, 128], P('blk', 'head'), may hold values from -6 to 6
- key_vectors: bfloat16 [8192, 128], P('blk'), may hold values from -6 to 6
- value_vectors: bfloat16 [8192, 128], P('blk'), may hold values from -6 to 6
- logsumexp: float32 [8192, 16], P('blk', 'head'), may hold values from 4 to 7
- positions: int32 [8192], P('blk'), may hold values from 0 to 8191, as said below
- doc_start: int32 [8192], P('blk'), may hold values from 0 to 8191, as said below
Outputs:
- query_grad: bfloat16 [8192, 16, 128], P('blk', 'head')
- key_grad: bfloat16 [8192, 128], P('blk')
- value_grad: bfloat16 [8192, 128], P('blk')
The draws below stay inside these ranges and needn't reach their ends.
Inputs may be any that keep to these rules, and one draw needn't show every extreme that they name: positions is a permutation of 0 to 8191; row r holds position (r mod 512) * 16 + sigma(r div 512), sigma a permutation of the blocks of 512 rows. doc_start of a row is the first position of the document that holds the row's position; documents are runs of consecutive positions, the first starting at 0, and the last position starts a document of its own.
All inputs are finite; a program needn't handle non-finite values.
Results may differ from the reference program's by a relative error of at most 0.0063.
Values may be sent and summed in bfloat16 or wider, within the bound.
No kernel may reach another device: no remote copies, remote signals or barrier semaphores. Data moves between devices by JAX's collectives and lax.ppermute only.
A program may use at most 64 MiB of HBM per device.

```python
import jax
import jax.numpy as jnp
from jax import lax

HQ = 16
HD = 128
TOK_DEV = 512
STEPS = 4
SEQ = 8192
N_BLK = 16


def shared_positions(key):
    sub_key = jax.random.fold_in(key, 11)
    block_order = jax.random.permutation(sub_key, N_BLK).astype(jnp.int32)
    row_ids = jnp.arange(SEQ, dtype=jnp.int32)
    return (row_ids % TOK_DEV * N_BLK + block_order[row_ids // TOK_DEV]).astype(jnp.int32)


def draw_positions(key, part):
    return shared_positions(key)


def draw_doc_start(key, part):
    places = shared_positions(key)
    doc_flags = jax.random.randint(jax.random.fold_in(key, 12), (SEQ,), 0, max(SEQ // 8, 2)) == 0
    cell_ids = jnp.arange(SEQ, dtype=jnp.int32)
    start_marks = jnp.where(doc_flags | (cell_ids == 0) | (cell_ids == SEQ - 1), cell_ids, 0).astype(jnp.int32)
    doc_starts = lax.cummax(start_marks, axis=0)
    return doc_starts[places].astype(jnp.int32)


def levels(key, shape, pieces, least, high):
    level, own = 1.0, jax.random.fold_in(key, 6)
    for axis_at, shards_of in pieces:
        steps = jnp.exp(jax.random.uniform(jax.random.fold_in(own, axis_at), (shards_of,), jnp.float32, least / len(pieces), high / len(pieces)))
        level = level * jnp.repeat(steps, shape[axis_at] // shards_of).reshape([-1 if axis == axis_at else 1 for axis in range(len(shape))])
    return level


def normal_values(rng, extent, width, reach, cuts=(), kind=jnp.bfloat16):
    result = width * jax.random.normal(rng, extent, jnp.float32)
    if cuts:
        result = result * levels(rng, extent, cuts, -0.22, 0.18)
    return jnp.clip(result, -reach, reach).astype(kind)


def setup_inputs(seed: int = 0) -> dict:
    key_of = jax.random.split(jax.random.key(seed), 9)
    return {
        "queries": normal_values(key_of[0], (SEQ, HQ, HD), 1.0, 6.0, ((0, 16), (1, 2))),
        "out_grad": normal_values(key_of[1], (SEQ, HQ, HD), 1.0, 6.0, ((0, 16), (1, 2))),
        "outputs": normal_values(key_of[2], (SEQ, HQ, HD), 1.0, 6.0, ((0, 16), (1, 2))),
        "key_vectors": normal_values(key_of[3], (SEQ, HD), 1.0, 6.0, ((0, 16),)),
        "value_vectors": normal_values(key_of[4], (SEQ, HD), 1.0, 6.0, ((0, 16),)),
        "logsumexp": jnp.clip(4.0 + 3.0 * jax.random.uniform(key_of[5], (SEQ, HQ), jnp.float32) ** levels(key_of[5], (SEQ, HQ), ((0, 16), (1, 2)), -0.2, 0.2), 4.0, 7.0),
        "positions": draw_positions(jax.random.fold_in(key_of[8], 71), 0),
        "doc_start": draw_doc_start(jax.random.fold_in(key_of[8], 71), 0),
    }


def block_grads(queries, out_grad, logsumexp, row_delta, query_places, query_starts, key_vectors, value_vectors, key_places):
    scaling = HD ** -0.5
    query_wide = queries.astype(jnp.float32)
    grad_wide = out_grad.astype(jnp.float32)
    key_wide = key_vectors.astype(jnp.float32)
    value_wide = value_vectors.astype(jnp.float32)
    scores = jnp.einsum("thd,kd->htk", query_wide, key_wide) * scaling
    allowed = (key_places[None, :] <= query_places[:, None]) & (key_places[None, :] >= query_starts[:, None])
    attend = jnp.where(allowed[None], jnp.exp(scores - logsumexp.T[:, :, None]), jnp.float32(0.0))
    attend_low = lax.optimization_barrier(attend.astype(jnp.bfloat16)).astype(jnp.float32)
    attend_grad = jnp.einsum("thd,kd->htk", grad_wide, value_wide)
    score_grad = attend * (attend_grad - row_delta.T[:, :, None])
    score_low = lax.optimization_barrier(score_grad.astype(jnp.bfloat16)).astype(jnp.float32)
    value_part = jnp.einsum("htk,thd->kd", attend_low, grad_wide)
    key_part = scaling * jnp.einsum("htk,thd->kd", score_low, query_wide)
    query_part = scaling * jnp.einsum("htk,kd->thd", score_low, key_wide)
    return query_part, key_part, value_part


def reference(queries, out_grad, outputs, key_vectors, value_vectors, logsumexp, positions, doc_start):
    row_delta = jnp.sum(out_grad.astype(jnp.float32) * outputs.astype(jnp.float32), axis=-1)
    query_blocks = queries.reshape(N_BLK, TOK_DEV, HQ, HD)
    grad_blocks = out_grad.reshape(N_BLK, TOK_DEV, HQ, HD)
    norm_blocks = logsumexp.reshape(N_BLK, TOK_DEV, HQ)
    delta_blocks = row_delta.reshape(N_BLK, TOK_DEV, HQ)
    place_blocks = positions.reshape(N_BLK, TOK_DEV)
    start_blocks = doc_start.reshape(N_BLK, TOK_DEV)
    key_blocks = key_vectors.reshape(N_BLK, TOK_DEV, HD)
    value_blocks = value_vectors.reshape(N_BLK, TOK_DEV, HD)
    query_total = jnp.zeros((N_BLK, TOK_DEV, HQ, HD), jnp.float32)
    key_total = jnp.zeros((N_BLK, TOK_DEV, HD), jnp.float32)
    value_total = jnp.zeros((N_BLK, TOK_DEV, HD), jnp.float32)

    def block_pass(inputs):
        return block_grads(*inputs)

    for cycle_step in range(STEPS):
        moved_keys = jnp.roll(key_blocks, -cycle_step, axis=0)
        moved_values = jnp.roll(value_blocks, -cycle_step, axis=0)
        moved_places = jnp.roll(place_blocks, -cycle_step, axis=0)
        query_part, key_part, value_part = lax.map(block_pass, (query_blocks, grad_blocks, norm_blocks, delta_blocks, place_blocks, start_blocks, moved_keys, moved_values, moved_places))
        query_total = query_total + query_part
        key_total = key_total + jnp.roll(key_part, cycle_step, axis=0)
        value_total = value_total + jnp.roll(value_part, cycle_step, axis=0)
    return (query_total.reshape(SEQ, HQ, HD).astype(jnp.bfloat16), key_total.reshape(SEQ, HD).astype(jnp.bfloat16), value_total.reshape(SEQ, HD).astype(jnp.bfloat16))
```

```python
import functools, math
import jax
import jax.numpy as jnp
from jax import lax
from jax.experimental import pallas as pl
from jax.experimental.pallas import tpu as pltpu
from jax.sharding import PartitionSpec as P

F32, BF16 = jnp.float32, jnp.bfloat16
NT = (((1,), (1,)), ((), ()))
TN = (((0,), (0,)), ((), ()))
TILE = 64
WIN = 128

def split3(x):
    a = x.astype(BF16); r = x - a.astype(F32)
    b = r.astype(BF16); r = r - b.astype(F32)
    return a, b, r.astype(BF16)

def kernel_body(nb, first, n_blk, heads, starts_ref, plane_ref, *refs):
    if first:
        (q_ref, g_ref, o_ref, tab_ref, *rest) = refs
        dq_out, vec_out, same_out, cross_out, kp, vp, dk_acc, dv_acc = rest[nb:]
        vec_ref = vec_out
    else:
        (q_ref, g_ref, vec_ref, dq_in, *rest) = refs
        dq_out, same_out, cross_out, kp, vp, dk_acc, dv_acc = rest[nb:]
    kv_refs = rest[:nb]
    hd = q_ref.shape[1]
    pad = WIN - TILE
    cols = TILE * heads
    tok = q_ref.shape[0] // heads
    c = hd ** -0.5 * math.log2(math.e)
    zero_pad = jnp.zeros((pad, hd), BF16)
    for b in range(nb):
        kp[b, :pad] = zero_pad
        vp[b, :pad] = zero_pad
        kp[b, pad:] = kv_refs[b][:tok]
        vp[b, pad:] = kv_refs[b][tok:2 * tok]
    dk_acc[...] = jnp.zeros_like(dk_acc)
    dv_acc[...] = jnp.zeros_like(dv_acc)
    sigs = [kv_refs[b][2 * tok:, :1].astype(F32) for b in range(nb)]

    def prep(i):
        rows = pl.ds(pl.multiple_of(i * cols, cols), cols)
        prod = g_ref[rows, :].astype(F32) * o_ref[rows, :].astype(F32)
        hi = prod.astype(BF16)
        lo = (prod - hi.astype(F32)).astype(BF16)
        ones = jnp.ones((8, 2 * hd), BF16)
        delta = lax.dot_general(ones, jnp.concatenate([hi, lo], axis=1), NT, preferred_element_type=F32)
        t = tab_ref[pl.ds(pl.multiple_of(i * TILE, TILE), TILE), :]
        w = t.shape[1]
        x = jnp.broadcast_to(t[:, None, :], (TILE, heads, w)).reshape(cols, w)
        lane = lax.broadcasted_iota(jnp.int32, (cols, w), 1)
        sub = lax.broadcasted_iota(jnp.int32, (cols, w), 0) % heads
        x = jnp.where((lane == sub) | (lane >= heads), x, 0.0)
        parts = split3(x)
        sel_row = lax.broadcasted_iota(jnp.int32, (16, w), 0)
        sel_lane = lax.broadcasted_iota(jnp.int32, (16, w), 1)
        sel = jnp.where((sel_row < 8) == (sel_lane < heads), 1.0, 0.0).astype(BF16)
        both = sum(lax.dot_general(sel, p_, NT, preferred_element_type=F32) for p_ in parts)
        vec_out[0:8, rows] = both[:8] * math.log2(math.e)
        vec_out[8:16, rows] = delta
        vec_out[16:24, rows] = both[8:]
        token = lax.broadcasted_iota(jnp.int32, (8, cols), 1) // heads + i * TILE
        vec_out[24:32, rows] = token.astype(F32) * n_blk + sigs[0][:8]

    def window(i, at, dq):
        rows = pl.ds(pl.multiple_of(i * cols, cols), cols)
        keys = pl.ds(pl.multiple_of(at, 64), WIN)
        qs, gs = q_ref[rows, :], g_ref[rows, :]
        kw = kp[:, keys, :].reshape(nb * WIN, hd)
        vw = vp[:, keys, :].reshape(nb * WIN, hd)
        lse = vec_ref[0:1, rows]
        delta = vec_ref[8:9, rows]
        begin = vec_ref[16:17, rows]
        s = lax.dot_general(kw, qs, NT, preferred_element_type=F32)
        dp = lax.dot_general(vw, gs, NT, preferred_element_type=F32)
        place = vec_ref[24:25, rows]
        key_row = (lax.broadcasted_iota(jnp.int32, (WIN, 1), 0) + (at - pad)).astype(F32) * n_blk
        key_place = jnp.concatenate([key_row + sg[:1] for sg in sigs], axis=0)
        ok = (key_place >= begin) & (key_place <= place)
        p = jnp.where(ok, jnp.exp2(s * c - lse), 0.0)
        ds = p * (dp - delta)
        p_low, ds_low = p.astype(BF16), ds.astype(BF16)
        dv = jnp.dot(p_low, gs, preferred_element_type=F32)
        dk = jnp.dot(ds_low, qs, preferred_element_type=F32)
        dv_acc[:, keys, :] += dv.reshape(nb, WIN, hd)
        dk_acc[:, keys, :] += dk.reshape(nb, WIN, hd)
        return dq + lax.dot_general(kw, ds_low, TN, preferred_element_type=F32)

    def tile(i, carry):
        rows = pl.ds(pl.multiple_of(i * cols, cols), cols)
        if first:
            prep(i)
            dq = jnp.zeros((hd, cols), F32)
        else:
            dq = dq_in[:, rows]
        dq = window(i, i * TILE, dq)
        low = starts_ref[i * TILE] // n_blk
        far = jnp.maximum((i - 1) * TILE - low + WIN - 1, 0) // WIN
        def more(w, dq):
            return window(i, jnp.maximum(i * TILE - (w + 1) * WIN, 0), dq)
        dq = lax.fori_loop(0, far, more, dq)
        if first:
            dq_out[:, rows] = dq
        else:
            dq_out[rows, :] = (dq * hd ** -0.5).T.astype(BF16)
        return carry

    lax.fori_loop(0, tok // TILE, tile, 0)
    keeps_keys = plane_ref[0] == 0
    for b in range(nb):
        dk = dk_acc[b, pad:] * hd ** -0.5
        dv = dv_acc[b, pad:]
        same_out[b] = jnp.where(keeps_keys, dk, dv).astype(same_out.dtype)
        cross_out[b] = jnp.where(keeps_keys, dv, dk).astype(cross_out.dtype)


def grads(nb, first, n_blk, heads, vmem_mib=40):
    def call(starts, plane, *args):
        rows, hd = args[0].shape
        tok = rows // heads
        vm = pl.BlockSpec(memory_space=pltpu.VMEM)
        S = jax.ShapeDtypeStruct
        outs = [S((hd, rows), F32), S((32, rows), F32)] if first else [S((rows, hd), BF16)]
        outs += [S((nb, tok, hd), F32 if first else BF16), S((nb, tok, hd), BF16)]
        pad = WIN - TILE
        return pl.pallas_call(
            functools.partial(kernel_body, nb, first, n_blk, heads),
            out_shape=outs,
            in_specs=[pl.BlockSpec(memory_space=pltpu.SMEM)] * 2 + [vm] * len(args),
            out_specs=[vm] * len(outs),
            scratch_shapes=[pltpu.VMEM((nb, tok + pad, hd), BF16)] * 2 + [pltpu.VMEM((nb, tok + pad, hd), F32)] * 2,
            compiler_params=pltpu.CompilerParams(vmem_limit_bytes=vmem_mib * 2**20),
            cost_estimate=pl.CostEstimate(flops=nb * tok * tok * heads * hd * 4, bytes_accessed=8 * 2**20, transcendentals=nb * tok * tok * heads // 2),
        )(starts, plane, *args)
    return call


def move(block, axes, pairs):
    return lax.ppermute(block, axes, pairs)


def on_device(queries, out_grad, outputs, keys, values, logsumexp, positions, doc_start):
    n = lax.axis_size("blk")
    tok, heads, hd = queries.shape
    devices = range(n)
    plane = lax.axis_index("head")
    kv = jnp.concatenate([keys, values, jnp.full((16, hd), positions[0], BF16)], axis=0)

    two_back = [(s, (s - 2) % n) for s in devices]
    odd_even = [(s, (s - 1) % n if s % 2 else (s - 3) % n) for s in devices]
    cores = [(s, s ^ 1) for s in devices]
    kv_a = move(kv, "blk", two_back)
    kv_b = move(kv, "blk", odd_even)
    kv_c = move(kv_a, "blk", cores)

    q, g, o = (x.reshape(tok * heads, hd) for x in (queries, out_grad, outputs))
    begin = doc_start.astype(F32)[:, None]
    table = jnp.concatenate([logsumexp, begin, jnp.zeros((tok, 7), F32)], axis=1)
    which = plane.astype(jnp.int32).reshape(1)
    dq, vec, own_same, own_cross = grads(1, True, n, heads)(doc_start, which, q, g, o, table, kv)
    dq, same, cross = grads(3, False, n, heads)(doc_start, which, q, g, vec, dq, kv_a, kv_b, kv_c)

    other = [(0, 1), (1, 0)]
    got = [move(own_cross[0], "head", other)]
    near = move(jnp.stack([same[2], cross[2]]), "blk", cores)
    both = lambda pairs, flip: [(2 * d + h, 2 * t + (h ^ flip)) for d, t in pairs for h in range(2)]
    back = lambda pairs: [(t, s) for s, t in pairs]
    got.append(move(same[0] + near[0], ("blk", "head"), both(back(two_back), 0)))
    got.append(move(cross[0] + near[1], ("blk", "head"), both(back(two_back), 1)))
    got.append(move(same[1], ("blk", "head"), both(back(odd_even), 0)))
    got.append(move(cross[1], ("blk", "head"), both(back(odd_even), 1)))
    total = own_same[0]
    for part in got:
        total = total + part.astype(F32)
    mine = total.astype(BF16)
    theirs = move(mine, "head", other)
    key_grad = jnp.where(plane == 0, mine, theirs)
    value_grad = jnp.where(plane == 0, theirs, mine)
    return dq.reshape(tok, heads, hd), key_grad, value_grad


def solution(mesh):
    in_specs = (
        P("blk", "head", None),
        P("blk", "head", None),
        P("blk", "head", None),
        P("blk", None),
        P("blk", None),
        P("blk", "head"),
        P("blk"),
        P("blk"),
    )
    out_specs = (P("blk", "head", None), P("blk", None), P("blk", None))
    return jax.shard_map(on_device, mesh=mesh, in_specs=in_specs, out_specs=out_specs, check_vma=False)
```

```python
import functools
import math

import jax
import jax.numpy as jnp
from jax import lax
from jax.experimental import pallas as pl
from jax.experimental.pallas import tpu as pltpu
from jax.sharding import PartitionSpec as P

F32, BF16 = jnp.float32, jnp.bfloat16
NT = (((1,), (1,)), ((), ()))
TN = (((0,), (0,)), ((), ()))
NN = (((1,), (0,)), ((), ()))
TILE = 64
WIN = 128
LOG2E = math.log2(math.e)


def dot(a, b, dims):
    return lax.dot_general(a, b, dims, preferred_element_type=F32)


def split3(x):
    high = x.astype(BF16)
    rest = x - high.astype(F32)
    mid = rest.astype(BF16)
    return high, mid, (rest - mid.astype(F32)).astype(BF16)


def columns(i, cols):
    return pl.ds(i * cols, cols)


def prep_kernel(
    q_hbm, g_hbm, o_hbm, places_hbm, starts_hbm, lse_hbm,
    vec_ref, q_ref, g_ref, o_ref, places_ref, starts_ref, lse_ref, sems, row_sems,
):
    heads, tok = lse_ref.shape
    hd = g_ref.shape[1]
    part = 128
    cols = part * heads
    pairs = ((g_hbm, g_ref), (o_hbm, o_ref), (q_hbm, q_ref))
    copies = [
        [
            pltpu.make_async_copy(src.at[columns(i, cols)], dst.at[columns(i, cols)], sems.at[m, i])
            for i in range(tok // part)
        ]
        for m, (src, dst) in enumerate(pairs)
    ]
    small = ((places_hbm, places_ref), (starts_hbm, starts_ref), (lse_hbm, lse_ref))
    small = [pltpu.make_async_copy(x, y, row_sems.at[m]) for m, (x, y) in enumerate(small)]
    for copy in small + copies[0] + copies[1] + copies[2]:
        copy.start()
    for copy in small:
        copy.wait()
    spread = lax.broadcasted_iota(jnp.int32, (part, cols), 1) // heads == lax.broadcasted_iota(
        jnp.int32, (part, cols), 0
    )
    spread = jnp.where(spread, 1.0, 0.0).astype(BF16)
    own = lax.broadcasted_iota(jnp.int32, (heads, cols), 1) % heads == lax.broadcasted_iota(
        jnp.int32, (heads, cols), 0
    )
    ones = jnp.ones((8, 2 * hd), BF16)
    for i in range(tok // part):
        rows, lanes = columns(i, cols), pl.ds(i * part, part)
        lse = sum(dot(x, spread, NN) for x in split3(lse_ref[:, lanes] * LOG2E))
        lse = jnp.sum(jnp.where(own, lse, 0.0), axis=0, keepdims=True)
        vec_ref[0:8, rows] = jnp.broadcast_to(lse, (8, cols))
        for at, ref in ((16, starts_ref), (24, places_ref)):
            row = jnp.broadcast_to(ref[:, lanes].astype(F32), (8, part))
            vec_ref[at : at + 8, rows] = sum(dot(x, spread, NN) for x in split3(row)[:2])
        copies[0][i].wait()
        copies[1][i].wait()
        prod = g_ref[rows, :].astype(F32) * o_ref[rows, :].astype(F32)
        high = prod.astype(BF16)
        low = (prod - high.astype(F32)).astype(BF16)
        vec_ref[8:16, rows] = dot(ones, jnp.concatenate([high, low], axis=1), NT)
    for copy in copies[2]:
        copy.wait()


def grads_kernel(nb, n_blk, starts_ref, vec_ref, q_ref, g_ref, *refs):
    ks, vs, places, refs = refs[:nb], refs[nb : 2 * nb], refs[2 * nb : 3 * nb], refs[3 * nb :]
    dq_ref, own_ref, c_ref, a_ref, b_ref, dk_acc, dv_acc = refs
    hd = q_ref.shape[1]
    tok = ks[0].shape[0]
    heads = q_ref.shape[0] // tok
    tiles = tok // TILE
    cols = TILE * heads
    scale = hd**-0.5
    dk_acc[...] = jnp.zeros_like(dk_acc)
    dv_acc[...] = jnp.zeros_like(dv_acc)

    def window(i, at, top):
        rows = columns(i, cols)
        keys = pl.ds(at, WIN)
        qs, gs = q_ref[rows, :], g_ref[rows, :]
        kw = jnp.concatenate([k[keys, :] for k in ks], axis=0)
        vw = jnp.concatenate([v[keys, :] for v in vs], axis=0)
        lse, delta = vec_ref[0:1, rows], vec_ref[8:9, rows]
        begin, place = vec_ref[16:17, rows], vec_ref[24:25, rows]
        s = dot(kw, qs, NT)
        dp = dot(vw, gs, NT)
        row = lax.broadcasted_iota(jnp.int32, (WIN, cols), 0) + at
        row_place = (row * n_blk).astype(F32)
        oks = []
        for p in places:
            first = p[0:1, 0:1].astype(F32)
            ok = row_place >= begin - first
            oks.append(ok & (row_place <= place - first if top is None else row < top))
        ok = jnp.concatenate(oks, axis=0)
        attend = jnp.where(ok, jnp.exp2(s * (scale * LOG2E) - lse), 0.0)
        low = (attend * (dp - delta)).astype(BF16)
        dv = dot(attend.astype(BF16), gs, NN)
        dk = dot(low, qs, NN)
        for b in range(nb):
            dv_acc[b, keys, :] += dv[b * WIN : (b + 1) * WIN]
            dk_acc[b, keys, :] += dk[b * WIN : (b + 1) * WIN]
        return dot(kw, low, TN)

    for i in range(tiles):
        dq_ref[:, columns(i, cols)] = window(i, max((i + 1) * TILE - WIN, 0), None)
    for i in range(tiles):
        top = (i + 1) * TILE - WIN
        if top <= 0:
            continue
        far = jnp.maximum(top - starts_ref[i * TILE] // n_blk + WIN - 1, 0) // WIN

        def more(w, carry, i=i, top=top):
            edge = top - w * WIN
            at = pl.multiple_of(jnp.maximum(edge - WIN, 0), TILE)
            dq_ref[:, columns(i, cols)] += window(i, at, edge)
            return carry

        lax.fori_loop(0, far, more, 0)

    for b, out in enumerate((own_ref, a_ref, b_ref, c_ref)):
        out[0] = (dk_acc[b] * scale).astype(out.dtype)
        out[1] = dv_acc[b].astype(out.dtype)


def finish_kernel(heads, dq_ref, out_ref):
    hd, rows = dq_ref.shape
    cols = TILE * heads
    for i in range(rows // cols):
        at = columns(i, cols)
        out_ref[at, :] = (dq_ref[:, at] * hd**-0.5).T.astype(BF16)


def call(body, outs, specs, scratch, flops, *args):
    vmem = pl.BlockSpec(memory_space=pltpu.VMEM)
    return pl.pallas_call(
        body,
        out_shape=outs,
        in_specs=specs + [vmem] * (len(args) - len(specs)),
        out_specs=jax.tree.map(lambda _: vmem, outs),
        scratch_shapes=scratch,
        compiler_params=pltpu.CompilerParams(vmem_limit_bytes=32 * 2**20),
        cost_estimate=pl.CostEstimate(flops=flops, bytes_accessed=4 * 2**20, transcendentals=0),
    )(*args)


def on_device(queries, out_grad, outputs, keys, values, logsumexp, positions, doc_start):
    n = lax.axis_size("blk")
    tok, heads, hd = queries.shape
    rows = tok * heads
    shape = jax.ShapeDtypeStruct
    blocks = range(n)

    two_back = [(s, (s - 2) % n) for s in blocks]
    odd_even = [(s, (s - 1) % n if s % 2 else (s - 3) % n) for s in blocks]
    cores = [(s, s ^ 1) for s in blocks]
    move = lambda group, pairs: tuple(lax.ppermute(x, "blk", pairs) for x in group)
    mine = (keys, values, positions)
    a = move(mine, two_back)
    b = move(mine, odd_even)

    q, g, o = (x.reshape(rows, hd) for x in (queries, out_grad, outputs))
    line = lambda x: x.reshape(1, tok)
    vec, q, g = call(
        prep_kernel,
        [shape((32, rows), F32)] + [shape((rows, hd), BF16)] * 2,
        [pl.BlockSpec(memory_space=pltpu.HBM)] * 6,
        [
            pltpu.VMEM((rows, hd), BF16),
            pltpu.VMEM((1, tok), jnp.int32),
            pltpu.VMEM((1, tok), jnp.int32),
            pltpu.VMEM((heads, tok), F32),
            pltpu.SemaphoreType.DMA((3, tok // 128)),
            pltpu.SemaphoreType.DMA((3,)),
        ],
        2**32,
        *(
            pltpu.with_memory_space_constraint(x, pltpu.HBM)
            for x in (q, g, o, line(positions), line(doc_start), logsumexp.T)
        ),
    )
    a, vec = lax.optimization_barrier((a, vec))
    c = move(a, cores)
    part = shape((2, tok, hd), BF16)
    groups = (mine, a, b, c)
    dq, own, c_part, a_part, b_part = call(
        functools.partial(grads_kernel, 4, n),
        [shape((hd, rows), F32), shape((2, tok, hd), F32), part, part, part],
        [pl.BlockSpec(memory_space=pltpu.SMEM)],
        [pltpu.VMEM((4, tok, hd), F32)] * 2,
        2**35,
        doc_start, vec, q, g, *(x[0] for x in groups), *(x[1] for x in groups), *(line(x[2]) for x in groups),
    )

    other = [(0, 1), (1, 0)]
    back = lambda x, pairs: lax.ppermute(x, "blk", [(d, s) for s, d in pairs])
    near = lax.ppermute(c_part, "blk", cores)
    from_b = back(b_part, odd_even)
    from_a = [back(a_part[i] + near[i], two_back) for i in range(2)]
    query_grad = call(
        functools.partial(finish_kernel, heads), shape((rows, hd), BF16), [], [], 2**32, dq
    )
    from_b, query_grad = lax.optimization_barrier((from_b, query_grad))
    halves, rests = [], []
    for i in range(2):
        if i:
            from_a[i], halves[0] = lax.optimization_barrier((from_a[i], halves[0]))
        half = own[i] + from_a[i].astype(F32) + from_b[i].astype(F32)
        halves.append(half.astype(BF16))
        rests.append(lax.ppermute(halves[i], "head", other))
    grads = []
    for i in range(2):
        grads.append((halves[i].astype(F32) + rests[i].astype(F32)).astype(BF16))
    key_grad, value_grad = grads
    return query_grad.reshape(tok, heads, hd), key_grad, value_grad


def solution(mesh):
    in_specs = (
        P("blk", "head", None),
        P("blk", "head", None),
        P("blk", "head", None),
        P("blk", None),
        P("blk", None),
        P("blk", "head"),
        P("blk"),
        P("blk"),
    )
    out_specs = (P("blk", "head", None), P("blk", None), P("blk", None))
    return jax.shard_map(
        on_device, mesh=mesh, in_specs=in_specs, out_specs=out_specs, check_vma=False
    )
```

```python
import functools
import math

import jax
import jax.numpy as jnp
from jax import lax
from jax.experimental import pallas as pl
from jax.experimental.pallas import tpu as pltpu
from jax.sharding import PartitionSpec as P

F32, BF16 = jnp.float32, jnp.bfloat16
NT = (((1,), (1,)), ((), ()))
TN = (((0,), (0,)), ((), ()))
NN = (((1,), (0,)), ((), ()))
TILE = 64
WIN = 128
LOG2E = math.log2(math.e)


def dot(a, b, dims):
    return lax.dot_general(a, b, dims, preferred_element_type=F32)


def split3(x):
    high = x.astype(BF16)
    rest = x - high.astype(F32)
    mid = rest.astype(BF16)
    return high, mid, (rest - mid.astype(F32)).astype(BF16)


def columns(i, cols):
    return pl.ds(i * cols, cols)


def prep_kernel(
    q_hbm, g_hbm, o_hbm, places_hbm, starts_hbm, lse_hbm,
    vec_ref, q_ref, g_ref, o_ref, places_ref, starts_ref, lse_ref, sems, row_sems,
):
    heads, tok = lse_ref.shape
    hd = g_ref.shape[1]
    part = 128
    cols = part * heads
    pairs = ((g_hbm, g_ref), (o_hbm, o_ref), (q_hbm, q_ref))
    copies = [
        [
            pltpu.make_async_copy(src.at[columns(i, cols)], dst.at[columns(i, cols)], sems.at[m, i])
            for i in range(tok // part)
        ]
        for m, (src, dst) in enumerate(pairs)
    ]
    small = ((places_hbm, places_ref), (starts_hbm, starts_ref), (lse_hbm, lse_ref))
    small = [pltpu.make_async_copy(x, y, row_sems.at[m]) for m, (x, y) in enumerate(small)]
    for copy in small + copies[0] + copies[1] + copies[2]:
        copy.start()
    for copy in small:
        copy.wait()
    spread = lax.broadcasted_iota(jnp.int32, (part, cols), 1) // heads == lax.broadcasted_iota(
        jnp.int32, (part, cols), 0
    )
    spread = jnp.where(spread, 1.0, 0.0).astype(BF16)
    own = lax.broadcasted_iota(jnp.int32, (heads, cols), 1) % heads == lax.broadcasted_iota(
        jnp.int32, (heads, cols), 0
    )
    ones = jnp.ones((8, 2 * hd), BF16)
    for i in range(tok // part):
        rows, lanes = columns(i, cols), pl.ds(i * part, part)
        lse = sum(dot(x, spread, NN) for x in split3(lse_ref[:, lanes] * LOG2E))
        lse = jnp.sum(jnp.where(own, lse, 0.0), axis=0, keepdims=True)
        vec_ref[0:8, rows] = jnp.broadcast_to(lse, (8, cols))
        for at, ref in ((16, starts_ref), (24, places_ref)):
            row = jnp.broadcast_to(ref[:, lanes].astype(F32), (8, part))
            vec_ref[at : at + 8, rows] = sum(dot(x, spread, NN) for x in split3(row)[:2])
        copies[0][i].wait()
        copies[1][i].wait()
        prod = g_ref[rows, :].astype(F32) * o_ref[rows, :].astype(F32)
        high = prod.astype(BF16)
        low = (prod - high.astype(F32)).astype(BF16)
        vec_ref[8:16, rows] = dot(ones, jnp.concatenate([high, low], axis=1), NT)
    for copy in copies[2]:
        copy.wait()


def grads_kernel(nb, n_blk, first, starts_ref, vec_ref, q_ref, g_ref, *refs):
    ks, vs, places, refs = refs[:nb], refs[nb : 2 * nb], refs[2 * nb : 3 * nb], refs[3 * nb :]
    if not first:
        dq_in, *refs = refs
    dq_ref, *outs, dk_acc, dv_acc = refs
    hd = q_ref.shape[1]
    tok = ks[0].shape[0]
    heads = q_ref.shape[0] // tok
    tiles = tok // TILE
    cols = TILE * heads
    scale = hd**-0.5
    dk_acc[...] = jnp.zeros_like(dk_acc)
    dv_acc[...] = jnp.zeros_like(dv_acc)

    def window(i, at, top):
        rows = columns(i, cols)
        keys = pl.ds(at, WIN)
        qs, gs = q_ref[rows, :], g_ref[rows, :]
        kw = jnp.concatenate([k[keys, :] for k in ks], axis=0)
        vw = jnp.concatenate([v[keys, :] for v in vs], axis=0)
        lse, delta = vec_ref[0:1, rows], vec_ref[8:9, rows]
        begin, place = vec_ref[16:17, rows], vec_ref[24:25, rows]
        s = dot(kw, qs, NT)
        dp = dot(vw, gs, NT)
        row = lax.broadcasted_iota(jnp.int32, (WIN, cols), 0) + at
        row_place = (row * n_blk).astype(F32)
        oks = []
        for p in places:
            first_place = p[0:1, 0:1].astype(F32)
            ok = row_place >= begin - first_place
            oks.append(ok & (row_place <= place - first_place if top is None else row < top))
        ok = jnp.concatenate(oks, axis=0)
        attend = jnp.where(ok, jnp.exp2(s * (scale * LOG2E) - lse), 0.0)
        low = (attend * (dp - delta)).astype(BF16)
        dv = dot(attend.astype(BF16), gs, NN)
        dk = dot(low, qs, NN)
        for b in range(nb):
            dv_acc[b, keys, :] += dv[b * WIN : (b + 1) * WIN]
            dk_acc[b, keys, :] += dk[b * WIN : (b + 1) * WIN]
        return dot(kw, low, TN)

    for i in range(tiles):
        rows = columns(i, cols)
        dq = window(i, max((i + 1) * TILE - WIN, 0), None)
        dq_ref[:, rows] = dq if first else dq_in[:, rows] + dq
    for i in range(tiles):
        top = (i + 1) * TILE - WIN
        if top <= 0:
            continue
        far = jnp.maximum(top - starts_ref[i * TILE] // n_blk + WIN - 1, 0) // WIN

        def more(w, carry, i=i, top=top):
            edge = top - w * WIN
            at = pl.multiple_of(jnp.maximum(edge - WIN, 0), math.gcd(TILE, WIN))
            dq_ref[:, columns(i, cols)] += window(i, at, edge)
            return carry

        lax.fori_loop(0, far, more, 0)

    for b, out in enumerate(outs):
        out[0] = (dk_acc[b] * scale).astype(out.dtype)
        out[1] = dv_acc[b].astype(out.dtype)


def finish_kernel(heads, dq_ref, out_ref):
    hd, rows = dq_ref.shape
    cols = TILE * heads
    for i in range(rows // cols):
        at = columns(i, cols)
        out_ref[at, :] = (dq_ref[:, at] * hd**-0.5).T.astype(BF16)


def call(body, outs, specs, scratch, flops, *args, **more):
    vmem = pl.BlockSpec(memory_space=pltpu.VMEM)
    return pl.pallas_call(
        body,
        out_shape=outs,
        in_specs=specs + [vmem] * (len(args) - len(specs)),
        out_specs=jax.tree.map(lambda _: vmem, outs),
        scratch_shapes=scratch,
        compiler_params=pltpu.CompilerParams(vmem_limit_bytes=32 * 2**20),
        cost_estimate=pl.CostEstimate(flops=flops, bytes_accessed=4 * 2**20, transcendentals=0),
        **more,
    )(*args)


def grads(n, types, flops, doc_start, vec, q, g, groups, dq=None):
    nb = len(groups)
    rows, hd = q.shape
    tok = groups[0][0].shape[0]
    shape = jax.ShapeDtypeStruct
    last = [] if dq is None else [dq]
    return call(
        functools.partial(grads_kernel, nb, n, dq is None),
        [shape((hd, rows), F32)] + [shape((2, tok, hd), t) for t in types],
        [pl.BlockSpec(memory_space=pltpu.SMEM)],
        [pltpu.VMEM((nb, tok, hd), F32)] * 2,
        flops,
        doc_start, vec, q, g, *(x[i].reshape(-1, x[i].shape[-1]) for i in range(3) for x in groups), *last,
        input_output_aliases={} if dq is None else {4 + 3 * nb: 0},
    )


def send(group, pairs):
    got = []
    for x in group:
        got.append(lax.ppermute(x, "blk", pairs))
    return tuple(got)


def on_device(queries, out_grad, outputs, keys, values, logsumexp, positions, doc_start):
    n = lax.axis_size("blk")
    tok, heads, hd = queries.shape
    rows = tok * heads
    shape = jax.ShapeDtypeStruct
    blocks = range(n)

    two_back = [(s, (s - 2) % n) for s in blocks]
    odd_even = [(s, (s - 1) % n if s % 2 else (s - 3) % n) for s in blocks]
    cores = [(s, s ^ 1) for s in blocks]
    mine = (keys, values, positions)
    a = send(mine, two_back)
    b = send(mine, odd_even)

    q, g, o = (x.reshape(rows, hd) for x in (queries, out_grad, outputs))
    line = lambda x: x.reshape(1, tok)
    vec, q, g = call(
        prep_kernel,
        [shape((32, rows), F32)] + [shape((rows, hd), BF16)] * 2,
        [pl.BlockSpec(memory_space=pltpu.HBM)] * 6,
        [
            pltpu.VMEM((rows, hd), BF16),
            pltpu.VMEM((1, tok), jnp.int32),
            pltpu.VMEM((1, tok), jnp.int32),
            pltpu.VMEM((heads, tok), F32),
            pltpu.SemaphoreType.DMA((3, tok // 128)),
            pltpu.SemaphoreType.DMA((3,)),
        ],
        2**32,
        *(
            pltpu.with_memory_space_constraint(x, pltpu.HBM)
            for x in (q, g, o, line(positions), line(doc_start), logsumexp.T)
        ),
    )
    a, vec = lax.optimization_barrier((a, vec))
    c = send(a, cores)
    dq, a_part = grads(n, [BF16], 2**33, doc_start, vec, q, g, [a])
    dq, b_part, c_part = grads(n, [BF16, BF16], 2**34, doc_start, vec, q, g, [b, c], dq)

    other = [(0, 1), (1, 0)]
    near = lax.ppermute(a_part, "blk", cores)
    b_part, c_part = lax.optimization_barrier((b_part, c_part))
    from_b = lax.ppermute(b_part, "blk", [(d, s) for s, d in odd_even])
    home = [(d, (d + 1) % n if d % 2 else (d + 3) % n) for d in blocks]
    from_a = list(send([c_part[i] + near[i] for i in range(2)], home))
    dq, own = grads(n, [F32], 2**33, doc_start, vec, q, g, [mine], dq)
    query_grad = call(
        functools.partial(finish_kernel, heads), shape((rows, hd), BF16), [], [], 2**32, dq
    )
    from_b, query_grad, own = lax.optimization_barrier((from_b, query_grad, own))
    halves, rests = [], []
    for i in range(2):
        if i:
            from_a[i], halves[0] = lax.optimization_barrier((from_a[i], halves[0]))
        half = own[i] + from_a[i].astype(F32) + from_b[i].astype(F32)
        halves.append(half.astype(BF16))
        rests.append(lax.ppermute(halves[i], "head", other))
    sums = []
    for i in range(2):
        sums.append((halves[i].astype(F32) + rests[i].astype(F32)).astype(BF16))
    key_grad, value_grad = sums
    return query_grad.reshape(tok, heads, hd), key_grad, value_grad


def solution(mesh):
    in_specs = (
        P("blk", "head", None),
        P("blk", "head", None),
        P("blk", "head", None),
        P("blk", None),
        P("blk", None),
        P("blk", "head"),
        P("blk"),
        P("blk"),
    )
    out_specs = (P("blk", "head", None), P("blk", None), P("blk", None))
    return jax.shard_map(
        on_device, mesh=mesh, in_specs=in_specs, out_specs=out_specs, check_vma=False
    )
```

```python
import functools
import math

import jax
import jax.numpy as jnp
from jax import lax
from jax.experimental import pallas as pl
from jax.experimental.pallas import tpu as pltpu
from jax.sharding import PartitionSpec as P

F32, BF16 = jnp.float32, jnp.bfloat16
NT = (((1,), (1,)), ((), ()))
TN = (((0,), (0,)), ((), ()))
NN = (((1,), (0,)), ((), ()))
TILE = 64
WIN = 128
LOG2E = math.log2(math.e)


def dot(a, b, dims):
    return lax.dot_general(a, b, dims, preferred_element_type=F32)


def split3(x):
    high = x.astype(BF16)
    rest = x - high.astype(F32)
    mid = rest.astype(BF16)
    return high, mid, (rest - mid.astype(F32)).astype(BF16)


def columns(i, cols):
    return pl.ds(i * cols, cols)


def prep_kernel(
    g_hbm, o_hbm, places_hbm, starts_hbm, lse_hbm,
    vec_ref, g_ref, o_ref, places_ref, starts_ref, lse_ref, sems, row_sems,
):
    heads, tok = lse_ref.shape
    hd = g_ref.shape[1]
    part = 128
    cols = part * heads
    pairs = ((g_hbm, g_ref), (o_hbm, o_ref))
    copies = [
        [
            pltpu.make_async_copy(src.at[columns(i, cols)], dst.at[columns(i, cols)], sems.at[m, i])
            for i in range(tok // part)
        ]
        for m, (src, dst) in enumerate(pairs)
    ]
    small = ((places_hbm, places_ref), (starts_hbm, starts_ref), (lse_hbm, lse_ref))
    small = [pltpu.make_async_copy(x, y, row_sems.at[m]) for m, (x, y) in enumerate(small)]
    for copy in small + [x for pair in zip(*copies) for x in pair]:
        copy.start()
    for copy in small:
        copy.wait()
    spread = lax.broadcasted_iota(jnp.int32, (part, cols), 1) // heads == lax.broadcasted_iota(
        jnp.int32, (part, cols), 0
    )
    spread = jnp.where(spread, 1.0, 0.0).astype(BF16)
    own = lax.broadcasted_iota(jnp.int32, (heads, cols), 1) % heads == lax.broadcasted_iota(
        jnp.int32, (heads, cols), 0
    )
    ones = jnp.ones((8, 2 * hd), BF16)
    for i in range(tok // part):
        rows, lanes = columns(i, cols), pl.ds(i * part, part)
        lse = sum(dot(x, spread, NN) for x in split3(lse_ref[:, lanes] * LOG2E))
        lse = jnp.sum(jnp.where(own, lse, 0.0), axis=0, keepdims=True)
        vec_ref[0:8, rows] = jnp.broadcast_to(lse, (8, cols))
        for at, ref in ((16, starts_ref), (24, places_ref)):
            row = jnp.broadcast_to(ref[:, lanes].astype(F32), (8, part))
            vec_ref[at : at + 8, rows] = sum(dot(x, spread, NN) for x in split3(row)[:2])
        copies[0][i].wait()
        copies[1][i].wait()
        prod = g_ref[rows, :].astype(F32) * o_ref[rows, :].astype(F32)
        high = prod.astype(BF16)
        low = (prod - high.astype(F32)).astype(BF16)
        vec_ref[8:16, rows] = dot(ones, jnp.concatenate([high, low], axis=1), NT)


def grads_kernel(nb, n_blk, first, starts_ref, vec_ref, q_ref, g_ref, *refs):
    ks, vs, places, refs = refs[:nb], refs[nb : 2 * nb], refs[2 * nb : 3 * nb], refs[3 * nb :]
    if not first:
        dq_in, *refs = refs
    dq_ref, *outs, dk_acc, dv_acc = refs
    hd = q_ref.shape[1]
    tok = ks[0].shape[0]
    heads = q_ref.shape[0] // tok
    tiles = tok // TILE
    cols = TILE * heads
    scale = hd**-0.5
    dk_acc[...] = jnp.zeros_like(dk_acc)
    dv_acc[...] = jnp.zeros_like(dv_acc)

    def scores(i, at):
        rows = columns(i, cols)
        keys = pl.ds(at, WIN)
        kw = jnp.concatenate([k[keys, :] for k in ks], axis=0)
        vw = jnp.concatenate([v[keys, :] for v in vs], axis=0)
        return dot(kw, q_ref[rows, :], NT), dot(vw, g_ref[rows, :], NT)

    def window(i, at, top, s, dp):
        rows = columns(i, cols)
        keys = pl.ds(at, WIN)
        qs, gs = q_ref[rows, :], g_ref[rows, :]
        kw = jnp.concatenate([k[keys, :] for k in ks], axis=0)
        lse, delta = vec_ref[0:1, rows], vec_ref[8:9, rows]
        begin, place = vec_ref[16:17, rows], vec_ref[24:25, rows]
        row = lax.broadcasted_iota(jnp.int32, (WIN, cols), 0) + at
        row_place = (row * n_blk).astype(F32)
        oks = []
        for p in places:
            first_place = p[0:1, 0:1].astype(F32)
            ok = row_place >= begin - first_place
            oks.append(ok & (row_place <= place - first_place if top is None else row < top))
        ok = jnp.concatenate(oks, axis=0)
        attend = jnp.where(ok, jnp.exp2(s * (scale * LOG2E) - lse), 0.0)
        low = (attend * (dp - delta)).astype(BF16)
        dv = dot(attend.astype(BF16), gs, NN)
        dk = dot(low, qs, NN)
        for b in range(nb):
            dv_acc[b, keys, :] += dv[b * WIN : (b + 1) * WIN]
            dk_acc[b, keys, :] += dk[b * WIN : (b + 1) * WIN]
        return dot(kw, low, TN)

    starts = [max((i + 1) * TILE - WIN, 0) for i in range(tiles)]
    ahead = scores(0, starts[0])
    for i in range(tiles):
        rows = columns(i, cols)
        now, ahead = ahead, scores(i + 1, starts[i + 1]) if i + 1 < tiles else None
        dq = window(i, starts[i], None, *now)
        dq_ref[:, rows] = dq if first else dq_in[:, rows] + dq
    for i in range(tiles):
        top = (i + 1) * TILE - WIN
        if top <= 0:
            continue
        far = jnp.maximum(top - starts_ref[i * TILE] // n_blk + WIN - 1, 0) // WIN

        def more(w, carry, i=i, top=top):
            edge = top - w * WIN
            at = pl.multiple_of(jnp.maximum(edge - WIN, 0), math.gcd(TILE, WIN))
            dq_ref[:, columns(i, cols)] += window(i, at, edge, *scores(i, at))
            return carry

        lax.fori_loop(0, far, more, 0)

    for b, out in enumerate(outs):
        out[0] = (dk_acc[b] * scale).astype(out.dtype)
        out[1] = dv_acc[b].astype(out.dtype)


def finish_kernel(heads, dq_ref, out_ref):
    hd, rows = dq_ref.shape
    cols = TILE * heads
    for i in range(rows // cols):
        at = columns(i, cols)
        out_ref[at, :] = (dq_ref[:, at] * hd**-0.5).T.astype(BF16)


def call(body, outs, specs, scratch, flops, *args, **more):
    vmem = pl.BlockSpec(memory_space=pltpu.VMEM)
    return pl.pallas_call(
        body,
        out_shape=outs,
        in_specs=specs + [vmem] * (len(args) - len(specs)),
        out_specs=jax.tree.map(lambda _: vmem, outs),
        scratch_shapes=scratch,
        compiler_params=pltpu.CompilerParams(vmem_limit_bytes=32 * 2**20),
        cost_estimate=pl.CostEstimate(flops=flops, bytes_accessed=4 * 2**20, transcendentals=0),
        **more,
    )(*args)


def grads(n, types, flops, doc_start, vec, q, g, groups, dq=None):
    nb = len(groups)
    rows, hd = q.shape
    tok = groups[0][0].shape[0]
    shape = jax.ShapeDtypeStruct
    last = [] if dq is None else [dq]
    return call(
        functools.partial(grads_kernel, nb, n, dq is None),
        [shape((hd, rows), F32)] + [shape((2, tok, hd), t) for t in types],
        [pl.BlockSpec(memory_space=pltpu.SMEM)],
        [pltpu.VMEM((nb, tok, hd), F32)] * 2,
        flops,
        doc_start, vec, q, g, *(x[i].reshape(-1, x[i].shape[-1]) for i in range(3) for x in groups), *last,
        input_output_aliases={} if dq is None else {4 + 3 * nb: 0},
    )


def send(group, pairs):
    got = []
    for x in group:
        got.append(lax.ppermute(x, "blk", pairs))
    return tuple(got)


def on_device(queries, out_grad, outputs, keys, values, logsumexp, positions, doc_start):
    n = lax.axis_size("blk")
    tok, heads, hd = queries.shape
    rows = tok * heads
    shape = jax.ShapeDtypeStruct
    blocks = range(n)

    two_back = [(s, (s - 2) % n) for s in blocks]
    odd_even = [(s, (s - 1) % n if s % 2 else (s - 3) % n) for s in blocks]
    cores = [(s, s ^ 1) for s in blocks]
    mine = (keys, values, positions)
    a = send(mine, two_back)
    b = send(mine, odd_even)

    q, g, o = (x.reshape(rows, hd) for x in (queries, out_grad, outputs))
    line = lambda x: x.reshape(1, tok)
    vec, g = call(
        prep_kernel,
        [shape((32, rows), F32), shape((rows, hd), BF16)],
        [pl.BlockSpec(memory_space=pltpu.HBM)] * 5,
        [
            pltpu.VMEM((rows, hd), BF16),
            pltpu.VMEM((1, tok), jnp.int32),
            pltpu.VMEM((1, tok), jnp.int32),
            pltpu.VMEM((heads, tok), F32),
            pltpu.SemaphoreType.DMA((2, tok // 128)),
            pltpu.SemaphoreType.DMA((3,)),
        ],
        2**32,
        *(
            pltpu.with_memory_space_constraint(x, pltpu.HBM)
            for x in (g, o, line(positions), line(doc_start), logsumexp.T)
        ),
    )
    a, vec = lax.optimization_barrier((a, vec))
    c = send(a, cores)
    dq, a_part = grads(n, [BF16], 2**33, doc_start, vec, q, g, [a])
    dq, c_part = grads(n, [BF16], 2**33, doc_start, vec, q, g, [c], dq)

    other = [(0, 1), (1, 0)]
    near = lax.ppermute(a_part, "blk", cores)
    home = [(d, (d + 1) % n if d % 2 else (d + 3) % n) for d in blocks]
    from_a = list(send([c_part[i] + near[i] for i in range(2)], home))
    dq, b_part = grads(n, [BF16], 2**33, doc_start, vec, q, g, [b], dq)
    from_b = send([b_part], [(d, s) for s, d in odd_even])[0]
    dq, own = grads(n, [F32], 2**33, doc_start, vec, q, g, [mine], dq)
    from_b, own = lax.optimization_barrier((from_b, own))
    query_grad = call(
        functools.partial(finish_kernel, heads), shape((rows, hd), BF16), [], [], 2**32, dq
    )
    halves, rests = [], []
    for i in range(2):
        if i:
            from_a[i], halves[0] = lax.optimization_barrier((from_a[i], halves[0]))
        half = own[i] + from_a[i].astype(F32) + from_b[i].astype(F32)
        halves.append(half.astype(BF16))
        rests.append(lax.ppermute(halves[i], "head", other))
    sums = []
    for i in range(2):
        sums.append((halves[i].astype(F32) + rests[i].astype(F32)).astype(BF16))
    key_grad, value_grad = sums
    return query_grad.reshape(tok, heads, hd), key_grad, value_grad


def solution(mesh):
    in_specs = (
        P("blk", "head", None),
        P("blk", "head", None),
        P("blk", "head", None),
        P("blk", None),
        P("blk", None),
        P("blk", "head"),
        P("blk"),
        P("blk"),
    )
    out_specs = (P("blk", "head", None), P("blk", None), P("blk", None))
    return jax.shard_map(
        on_device, mesh=mesh, in_specs=in_specs, out_specs=out_specs, check_vma=False
    )
```

```python
import functools
import math

import jax
import jax.numpy as jnp
from jax import lax
from jax.experimental import pallas as pl
from jax.experimental.pallas import tpu as pltpu
from jax.sharding import PartitionSpec as P

F32, BF16 = jnp.float32, jnp.bfloat16
NT = (((1,), (1,)), ((), ()))
TN = (((0,), (0,)), ((), ()))
NN = (((1,), (0,)), ((), ()))
TILE = 64
WIN = 128
LOG2E = math.log2(math.e)


def dot(a, b, dims):
    return lax.dot_general(a, b, dims, preferred_element_type=F32)


def split3(x):
    high = x.astype(BF16)
    rest = x - high.astype(F32)
    mid = rest.astype(BF16)
    return high, mid, (rest - mid.astype(F32)).astype(BF16)


def columns(i, cols):
    return pl.ds(i * cols, cols)


def prep_kernel(
    g_hbm, o_hbm, places_hbm, starts_hbm, lse_hbm,
    vec_ref, g_ref, o_ref, places_ref, starts_ref, lse_ref, sems, row_sems,
):
    heads, tok = lse_ref.shape
    hd = g_ref.shape[1]
    part = 128
    cols = part * heads
    pairs = ((g_hbm, g_ref), (o_hbm, o_ref))
    copies = [
        [
            pltpu.make_async_copy(src.at[columns(i, cols)], dst.at[columns(i, cols)], sems.at[m, i])
            for i in range(tok // part)
        ]
        for m, (src, dst) in enumerate(pairs)
    ]
    small = ((places_hbm, places_ref), (starts_hbm, starts_ref), (lse_hbm, lse_ref))
    small = [pltpu.make_async_copy(x, y, row_sems.at[m]) for m, (x, y) in enumerate(small)]
    for i, copy in enumerate(small + [x for pair in zip(*copies) for x in pair]):
        copy.start(priority=i % 2)
    for copy in small:
        copy.wait()
    spread = lax.broadcasted_iota(jnp.int32, (part, cols), 1) // heads == lax.broadcasted_iota(
        jnp.int32, (part, cols), 0
    )
    spread = jnp.where(spread, 1.0, 0.0).astype(BF16)
    own = lax.broadcasted_iota(jnp.int32, (heads, cols), 1) % heads == lax.broadcasted_iota(
        jnp.int32, (heads, cols), 0
    )
    ones = jnp.ones((8, 2 * hd), BF16)
    for i in range(tok // part):
        rows, lanes = columns(i, cols), pl.ds(i * part, part)
        lse = sum(dot(x, spread, NN) for x in split3(lse_ref[:, lanes] * LOG2E))
        lse = jnp.sum(jnp.where(own, lse, 0.0), axis=0, keepdims=True)
        vec_ref[0:8, rows] = jnp.broadcast_to(lse, (8, cols))
        for at, ref in ((16, starts_ref), (24, places_ref)):
            row = jnp.broadcast_to(ref[:, lanes].astype(F32), (8, part))
            vec_ref[at : at + 8, rows] = sum(dot(x, spread, NN) for x in split3(row)[:2])
        copies[0][i].wait()
        copies[1][i].wait()
        prod = g_ref[rows, :].astype(F32) * o_ref[rows, :].astype(F32)
        high = prod.astype(BF16)
        low = (prod - high.astype(F32)).astype(BF16)
        vec_ref[8:16, rows] = dot(ones, jnp.concatenate([high, low], axis=1), NT)


def grads_kernel(nb, n_blk, starts_ref, vec_ref, q_ref, g_ref, *refs):
    ks, vs, places, refs = refs[:nb], refs[nb : 2 * nb], refs[2 * nb : 3 * nb], refs[3 * nb :]
    dq_ref, *outs, dk_acc, dv_acc = refs
    hd = q_ref.shape[1]
    tok = ks[0].shape[0]
    heads = q_ref.shape[0] // tok
    tiles = tok // TILE
    cols = TILE * heads
    scale = hd**-0.5
    dk_acc[...] = jnp.zeros_like(dk_acc)
    dv_acc[...] = jnp.zeros_like(dv_acc)

    def scores(i, at):
        rows = columns(i, cols)
        keys = pl.ds(at, WIN)
        kw = jnp.concatenate([k[keys, :] for k in ks], axis=0)
        vw = jnp.concatenate([v[keys, :] for v in vs], axis=0)
        return dot(kw, q_ref[rows, :], NT), dot(vw, g_ref[rows, :], NT)

    def window(i, at, top, s, dp):
        rows = columns(i, cols)
        keys = pl.ds(at, WIN)
        qs, gs = q_ref[rows, :], g_ref[rows, :]
        kw = jnp.concatenate([k[keys, :] for k in ks], axis=0)
        lse, delta = vec_ref[0:1, rows], vec_ref[8:9, rows]
        begin, place = vec_ref[16:17, rows], vec_ref[24:25, rows]
        row = lax.broadcasted_iota(jnp.int32, (WIN, cols), 0) + at
        row_place = (row * n_blk).astype(F32)
        oks = []
        for p in places:
            first_place = p[0:1, 0:1].astype(F32)
            ok = row_place >= begin - first_place
            oks.append(ok & (row_place <= place - first_place if top is None else row < top))
        ok = jnp.concatenate(oks, axis=0)
        attend = jnp.where(ok, jnp.exp2(s * (scale * LOG2E) - lse), 0.0)
        low = (attend * (dp - delta)).astype(BF16)
        dv = dot(attend.astype(BF16), gs, NN)
        dk = dot(low, qs, NN)
        for b in range(nb):
            dv_acc[b, keys, :] += dv[b * WIN : (b + 1) * WIN]
            dk_acc[b, keys, :] += dk[b * WIN : (b + 1) * WIN]
        return dot(kw, low, TN)

    starts = [max((i + 1) * TILE - WIN, 0) for i in range(tiles)]
    ahead = scores(0, starts[0])
    for i in range(tiles):
        rows = columns(i, cols)
        now, ahead = ahead, scores(i + 1, starts[i + 1]) if i + 1 < tiles else None
        dq_ref[:, rows] = window(i, starts[i], None, *now)
    for i in range(tiles):
        top = (i + 1) * TILE - WIN
        if top <= 0:
            continue
        far = jnp.maximum(top - starts_ref[i * TILE] // n_blk + WIN - 1, 0) // WIN

        def more(w, carry, i=i, top=top):
            edge = top - w * WIN
            at = pl.multiple_of(jnp.maximum(edge - WIN, 0), math.gcd(TILE, WIN))
            dq_ref[:, columns(i, cols)] += window(i, at, edge, *scores(i, at))
            return carry

        lax.fori_loop(0, far, more, 0)

    if len(outs) > nb:
        outs = [jax.tree.map(lambda x: x.at[0], outs)]
    for b, out in enumerate(outs):
        for at, x in ((0, dk_acc[b] * scale), (1, dv_acc[b])):
            part = out[at] if isinstance(out, list) else out.at[at]
            part[...] = x.astype(part.dtype)


def finish_kernel(heads, *refs):
    *parts, out_ref = refs
    rows, hd = out_ref.shape
    cols = TILE * heads
    for i in range(rows // cols):
        at = columns(i, cols)
        out_ref[at, :] = (sum(x[:, at] for x in parts) * hd**-0.5).T.astype(BF16)


def call(body, outs, specs, scratch, flops, *args):
    vmem = pl.BlockSpec(memory_space=pltpu.VMEM)
    return pl.pallas_call(
        body,
        out_shape=outs,
        in_specs=specs + [vmem] * (len(args) - len(specs)),
        out_specs=jax.tree.map(lambda _: vmem, outs),
        scratch_shapes=scratch,
        compiler_params=pltpu.CompilerParams(vmem_limit_bytes=32 * 2**20),
        cost_estimate=pl.CostEstimate(flops=flops, bytes_accessed=4 * 2**20, transcendentals=0),
    )(*args)


def grads(n, types, flops, doc_start, vec, q, g, groups, split=False):
    nb = len(groups)
    rows, hd = q.shape
    tok = groups[0][0].shape[0]
    shape = jax.ShapeDtypeStruct
    return call(
        functools.partial(grads_kernel, nb, n),
        [shape((hd, rows), F32)]
        + [shape((1, tok, hd) if split else (2, tok, hd), t) for t in types for _ in range(2 if split else 1)],
        [pl.BlockSpec(memory_space=pltpu.SMEM)],
        [pltpu.VMEM((nb, tok, hd), F32)] * 2,
        flops,
        doc_start, vec, q, g, *(x[i].reshape(-1, x[i].shape[-1]) for i in range(3) for x in groups),
    )


def send(group, pairs):
    got = []
    for x in group:
        got.append(lax.ppermute(x, "blk", pairs))
    return tuple(got)


def on_device(queries, out_grad, outputs, keys, values, logsumexp, positions, doc_start):
    n = lax.axis_size("blk")
    tok, heads, hd = queries.shape
    rows = tok * heads
    shape = jax.ShapeDtypeStruct
    blocks = range(n)

    two_back = [(s, (s - 2) % n) for s in blocks]
    odd_even = [(s, (s - 1) % n if s % 2 else (s - 3) % n) for s in blocks]
    cores = [(s, s ^ 1) for s in blocks]
    mine = (keys, values, positions)
    a = send(mine, two_back)
    b = send(mine, odd_even)

    q, g, o = (x.reshape(rows, hd) for x in (queries, out_grad, outputs))
    line = lambda x: x.reshape(1, tok)
    vec, g = call(
        prep_kernel,
        [shape((32, rows), F32), shape((rows, hd), BF16)],
        [pl.BlockSpec(memory_space=pltpu.HBM)] * 5,
        [
            pltpu.VMEM((rows, hd), BF16),
            pltpu.VMEM((1, tok), jnp.int32),
            pltpu.VMEM((1, tok), jnp.int32),
            pltpu.VMEM((heads, tok), F32),
            pltpu.SemaphoreType.DMA((2, tok // 128)),
            pltpu.SemaphoreType.DMA((3,)),
        ],
        2**32,
        *(
            pltpu.with_memory_space_constraint(x, pltpu.HBM)
            for x in (g, o, line(positions), line(doc_start), logsumexp.T)
        ),
    )
    a, vec = lax.optimization_barrier((a, vec))
    c = send(a, cores)
    dq_a, a_part = grads(n, [BF16], 2**33, doc_start, vec, q, g, [a])
    dq_c, c_part = grads(n, [BF16], 2**33, doc_start, vec, q, g, [c])

    other = [(0, 1), (1, 0)]
    near = lax.ppermute(a_part, "blk", cores)
    home = [(d, (d + 1) % n if d % 2 else (d + 3) % n) for d in blocks]
    from_a = list(send([c_part[i] + near[i] for i in range(2)], home))
    dq_b, *b_parts = grads(n, [BF16], 2**33, doc_start, vec, q, g, [b], split=True)
    from_b = list(send(b_parts, [(d, s) for s, d in odd_even]))
    dq_own, own = grads(n, [F32], 2**33, doc_start, vec, q, g, [mine])
    from_b[0], own = lax.optimization_barrier((from_b[0], own))
    query_grad = call(
        functools.partial(finish_kernel, heads), shape((rows, hd), BF16), [], [], 2**32,
        dq_a, dq_c, dq_b, dq_own,
    )
    halves, rests = [], []
    for i in range(2):
        if i:
            from_b[i], from_a[i], halves[0] = lax.optimization_barrier((from_b[i], from_a[i], halves[0]))
        half = own[i] + from_a[i].astype(F32) + from_b[i].reshape(tok, hd).astype(F32)
        halves.append(half.astype(BF16))
        rests.append(lax.ppermute(halves[i], "head", other))
    sums = []
    for i in range(2):
        sums.append((halves[i].astype(F32) + rests[i].astype(F32)).astype(BF16))
    key_grad, value_grad = sums
    return query_grad.reshape(tok, heads, hd), key_grad, value_grad


def solution(mesh):
    in_specs = (
        P("blk", "head", None),
        P("blk", "head", None),
        P("blk", "head", None),
        P("blk", None),
        P("blk", None),
        P("blk", "head"),
        P("blk"),
        P("blk"),
    )
    out_specs = (P("blk", "head", None), P("blk", None), P("blk", None))
    return jax.shard_map(
        on_device, mesh=mesh, in_specs=in_specs, out_specs=out_specs, check_vma=False
    )
```

```python
import functools
import math

import jax
import jax.numpy as jnp
from jax import lax
from jax.experimental import pallas as pl
from jax.experimental.pallas import tpu as pltpu
from jax.sharding import PartitionSpec as P

F32, BF16 = jnp.float32, jnp.bfloat16
NT = (((1,), (1,)), ((), ()))
TN = (((0,), (0,)), ((), ()))
NN = (((1,), (0,)), ((), ()))
TILE = 64
WIN = 192
LOG2E = math.log2(math.e)


def dot(a, b, dims):
    return lax.dot_general(a, b, dims, preferred_element_type=F32)


def split3(x):
    high = x.astype(BF16)
    rest = x - high.astype(F32)
    mid = rest.astype(BF16)
    return high, mid, (rest - mid.astype(F32)).astype(BF16)


def columns(i, cols):
    return pl.ds(i * cols, cols)


def prep_kernel(
    g_hbm, o_hbm, places_hbm, starts_hbm, lse_hbm,
    vec_ref, g_ref, o_ref, places_ref, starts_ref, lse_ref, sems, row_sems,
):
    heads, tok = lse_ref.shape
    hd = g_ref.shape[1]
    part = 128
    cols = part * heads
    pairs = ((g_hbm, g_ref), (o_hbm, o_ref))
    copies = [
        [
            pltpu.make_async_copy(src.at[columns(i, cols)], dst.at[columns(i, cols)], sems.at[m, i])
            for i in range(tok // part)
        ]
        for m, (src, dst) in enumerate(pairs)
    ]
    small = ((places_hbm, places_ref), (starts_hbm, starts_ref), (lse_hbm, lse_ref))
    small = [pltpu.make_async_copy(x, y, row_sems.at[m]) for m, (x, y) in enumerate(small)]
    for i, copy in enumerate(small + [x for pair in zip(*copies) for x in pair]):
        copy.start(priority=i % 2)
    for copy in small:
        copy.wait()
    spread = lax.broadcasted_iota(jnp.int32, (part, cols), 1) // heads == lax.broadcasted_iota(
        jnp.int32, (part, cols), 0
    )
    spread = jnp.where(spread, 1.0, 0.0).astype(BF16)
    own = lax.broadcasted_iota(jnp.int32, (heads, cols), 1) % heads == lax.broadcasted_iota(
        jnp.int32, (heads, cols), 0
    )
    ones = jnp.ones((8, 2 * hd), BF16)
    for i in range(tok // part):
        rows, lanes = columns(i, cols), pl.ds(i * part, part)
        lse = sum(dot(x, spread, NN) for x in split3(lse_ref[:, lanes] * LOG2E))
        lse = jnp.sum(jnp.where(own, lse, 0.0), axis=0, keepdims=True)
        vec_ref[0:8, rows] = jnp.broadcast_to(lse, (8, cols))
        for at, ref in ((16, starts_ref), (24, places_ref)):
            row = jnp.broadcast_to(ref[:, lanes].astype(F32), (8, part))
            vec_ref[at : at + 8, rows] = sum(dot(x, spread, NN) for x in split3(row)[:2])
        copies[0][i].wait()
        copies[1][i].wait()
        prod = g_ref[rows, :].astype(F32) * o_ref[rows, :].astype(F32)
        high = prod.astype(BF16)
        low = (prod - high.astype(F32)).astype(BF16)
        vec_ref[8:16, rows] = dot(ones, jnp.concatenate([high, low], axis=1), NT)


def grads_kernel(nb, n_blk, starts_ref, vec_ref, q_ref, g_ref, *refs):
    ks, vs, places, refs = refs[:nb], refs[nb : 2 * nb], refs[2 * nb : 3 * nb], refs[3 * nb :]
    dq_ref, *outs, dk_acc, dv_acc = refs
    hd = q_ref.shape[1]
    tok = ks[0].shape[0]
    heads = q_ref.shape[0] // tok
    tiles = tok // TILE
    cols = TILE * heads
    scale = hd**-0.5
    dk_acc[...] = jnp.zeros_like(dk_acc)
    dv_acc[...] = jnp.zeros_like(dv_acc)

    def scores(i, at, size):
        rows = columns(i, cols)
        keys = pl.ds(at, size)
        kw = jnp.concatenate([k[keys, :] for k in ks], axis=0)
        vw = jnp.concatenate([v[keys, :] for v in vs], axis=0)
        return dot(kw, q_ref[rows, :], NT), dot(vw, g_ref[rows, :], NT)

    def window(i, at, size, top, s, dp):
        rows = columns(i, cols)
        keys = pl.ds(at, size)
        qs, gs = q_ref[rows, :], g_ref[rows, :]
        kw = jnp.concatenate([k[keys, :] for k in ks], axis=0)
        lse, delta = vec_ref[0:1, rows], vec_ref[8:9, rows]
        begin, place = vec_ref[16:17, rows], vec_ref[24:25, rows]
        row = lax.broadcasted_iota(jnp.int32, (size, cols), 0) + at
        row_place = (row * n_blk).astype(F32)
        oks = []
        for p in places:
            first_place = p[0:1, 0:1].astype(F32)
            ok = row_place >= begin - first_place
            oks.append(ok & (row_place <= place - first_place if top is None else row < top))
        ok = jnp.concatenate(oks, axis=0)
        attend = jnp.where(ok, jnp.exp2(s * (scale * LOG2E) - lse), 0.0)
        low = (attend * (dp - delta)).astype(BF16)
        dv = dot(attend.astype(BF16), gs, NN)
        dk = dot(low, qs, NN)
        for b in range(nb):
            dv_acc[b, keys, :] += dv[b * size : (b + 1) * size]
            dk_acc[b, keys, :] += dk[b * size : (b + 1) * size]
        return dot(kw, low, TN)

    spans = [(max((i + 1) * TILE - WIN, 0), min((i + 1) * TILE, WIN)) for i in range(tiles)]
    ahead = scores(0, *spans[0])
    for i in range(tiles):
        rows = columns(i, cols)
        now, ahead = ahead, scores(i + 1, *spans[i + 1]) if i + 1 < tiles else None
        dq_ref[:, rows] = window(i, *spans[i], None, *now)
    for i in range(tiles):
        top = (i + 1) * TILE - WIN
        if top <= 0:
            continue
        far = jnp.maximum(top - starts_ref[i * TILE] // n_blk + WIN - 1, 0) // WIN

        def more(w, carry, i=i, top=top):
            edge = top - w * WIN
            at = pl.multiple_of(jnp.maximum(edge - WIN, 0), math.gcd(TILE, WIN))
            dq_ref[:, columns(i, cols)] += window(i, at, WIN, edge, *scores(i, at, WIN))
            return carry

        lax.fori_loop(0, far, more, 0)

    if len(outs) > nb:
        outs = [jax.tree.map(lambda x: x.at[0], outs)]
    for b, out in enumerate(outs):
        for at, x in ((0, dk_acc[b] * scale), (1, dv_acc[b])):
            part = out[at] if isinstance(out, list) else out.at[at]
            part[...] = x.astype(part.dtype)


def finish_kernel(heads, *refs):
    *parts, out_ref = refs
    rows, hd = out_ref.shape
    cols = TILE * heads
    for i in range(rows // cols):
        at = columns(i, cols)
        out_ref[at, :] = (sum(x[:, at] for x in parts) * hd**-0.5).T.astype(BF16)


def call(body, outs, specs, scratch, flops, *args):
    vmem = pl.BlockSpec(memory_space=pltpu.VMEM)
    return pl.pallas_call(
        body,
        out_shape=outs,
        in_specs=specs + [vmem] * (len(args) - len(specs)),
        out_specs=jax.tree.map(lambda _: vmem, outs),
        scratch_shapes=scratch,
        compiler_params=pltpu.CompilerParams(vmem_limit_bytes=32 * 2**20),
        cost_estimate=pl.CostEstimate(flops=flops, bytes_accessed=4 * 2**20, transcendentals=0),
    )(*args)


def grads(n, types, flops, doc_start, vec, q, g, groups, split=False):
    nb = len(groups)
    rows, hd = q.shape
    tok = groups[0][0].shape[0]
    shape = jax.ShapeDtypeStruct
    return call(
        functools.partial(grads_kernel, nb, n),
        [shape((hd, rows), F32)]
        + [shape((1, tok, hd) if split else (2, tok, hd), t) for t in types for _ in range(2 if split else 1)],
        [pl.BlockSpec(memory_space=pltpu.SMEM)],
        [pltpu.VMEM((nb, tok, hd), F32)] * 2,
        flops,
        doc_start, vec, q, g, *(x[i].reshape(-1, x[i].shape[-1]) for i in range(3) for x in groups),
    )


def send(group, pairs):
    got = []
    for x in group:
        got.append(lax.ppermute(x, "blk", pairs))
    return tuple(got)


def on_device(queries, out_grad, outputs, keys, values, logsumexp, positions, doc_start):
    n = lax.axis_size("blk")
    tok, heads, hd = queries.shape
    rows = tok * heads
    shape = jax.ShapeDtypeStruct
    blocks = range(n)

    two_back = [(s, (s - 2) % n) for s in blocks]
    odd_even = [(s, (s - 1) % n if s % 2 else (s - 3) % n) for s in blocks]
    cores = [(s, s ^ 1) for s in blocks]
    mine = (keys, values, positions)
    a = send(mine, two_back)
    b = send(mine, odd_even)

    q, g, o = (x.reshape(rows, hd) for x in (queries, out_grad, outputs))
    line = lambda x: x.reshape(1, tok)
    vec, g = call(
        prep_kernel,
        [shape((32, rows), F32), shape((rows, hd), BF16)],
        [pl.BlockSpec(memory_space=pltpu.HBM)] * 5,
        [
            pltpu.VMEM((rows, hd), BF16),
            pltpu.VMEM((1, tok), jnp.int32),
            pltpu.VMEM((1, tok), jnp.int32),
            pltpu.VMEM((heads, tok), F32),
            pltpu.SemaphoreType.DMA((2, tok // 128)),
            pltpu.SemaphoreType.DMA((3,)),
        ],
        2**32,
        *(
            pltpu.with_memory_space_constraint(x, pltpu.HBM)
            for x in (g, o, line(positions), line(doc_start), logsumexp.T)
        ),
    )
    a, vec = lax.optimization_barrier((a, vec))
    c = send(a, cores)
    dq_a, a_part = grads(n, [BF16], 2**33, doc_start, vec, q, g, [a])
    dq_c, c_part = grads(n, [BF16], 2**33, doc_start, vec, q, g, [c])

    other = [(0, 1), (1, 0)]
    near = lax.ppermute(a_part, "blk", cores)
    home = [(d, (d + 1) % n if d % 2 else (d + 3) % n) for d in blocks]
    from_a = list(send([c_part[i] + near[i] for i in range(2)], home))
    dq_b, *b_parts = grads(n, [BF16], 2**33, doc_start, vec, q, g, [b], split=True)
    from_b = list(send(b_parts, [(d, s) for s, d in odd_even]))
    dq_own, own = grads(n, [F32], 2**33, doc_start, vec, q, g, [mine])
    from_b[0], own = lax.optimization_barrier((from_b[0], own))
    query_grad = call(
        functools.partial(finish_kernel, heads), shape((rows, hd), BF16), [], [], 2**32,
        dq_a, dq_c, dq_b, dq_own,
    )
    halves, rests = [], []
    for i in range(2):
        if i:
            from_b[i], from_a[i], halves[0] = lax.optimization_barrier((from_b[i], from_a[i], halves[0]))
        half = own[i] + from_a[i].astype(F32) + from_b[i].reshape(tok, hd).astype(F32)
        halves.append(half.astype(BF16))
        rests.append(lax.ppermute(halves[i], "head", other))
    sums = []
    for i in range(2):
        sums.append((halves[i].astype(F32) + rests[i].astype(F32)).astype(BF16))
    key_grad, value_grad = sums
    return query_grad.reshape(tok, heads, hd), key_grad, value_grad


def solution(mesh):
    in_specs = (
        P("blk", "head", None),
        P("blk", "head", None),
        P("blk", "head", None),
        P("blk", None),
        P("blk", None),
        P("blk", "head"),
        P("blk"),
        P("blk"),
    )
    out_specs = (P("blk", "head", None), P("blk", None), P("blk", None))
    return jax.shard_map(
        on_device, mesh=mesh, in_specs=in_specs, out_specs=out_specs, check_vma=False
    )
```
